256 devices in a mesh: wide: 16 (over y, x_hi, core), narrow: 16 (over x_lo, z).
Axes of the slice: x: 4 (x_hi: 2, x_lo: 2; x = x_hi * 2 + x_lo), y: 4, z: 8, core: 2. Of those that a mesh axis runs over, the one named last changes fastest.
Arguments:
- left: bfloat16 [32, 32, 2048], P('narrow', None, 'wide'), may hold values from -6 to 6
- right: bfloat16 [32, 32, 2048], P('wide', None, 'narrow'), may hold values from -6 to 6
- out_weight: bfloat16 [1024, 128], replicated, may hold values from -1 to 1
- out_bias: float32 [128], replicated, may hold values from -3 to 3
- cotangent: bfloat16 [2048, 2048, 128], P('wide', 'narrow'), may hold values from -0.5 to 0.5
Outputs:
- pair_update: bfloat16 [2048, 2048, 128], P('wide', 'narrow')
- grad_left: float32 [32, 32, 2048], P('narrow', None, 'wide')
- grad_right: float32 [32, 32, 2048], P('wide', None, 'narrow')
The draws below stay inside these ranges and needn't reach their ends.
All inputs are finite; a program needn't handle non-finite values.
Results may differ from the reference program's by a relative error of at most 0.0045.
Values may be sent and summed in bfloat16 or wider, within the bound.
A program may use at most 64 MiB of HBM per device.

```python
import math
import jax
import jax.numpy as jnp
from jax import lax

C = 32
K = 128
S = 32
R = 2048


def level_of(own_key, dims, split, low, high):
    loudness = 1.0
    for position, shards_of in split:
        draws = jax.random.uniform(jax.random.fold_in(jax.random.fold_in(own_key, 6), position), (shards_of,), jnp.float32, low / len(split), high / len(split))
        loudness = loudness * jnp.repeat(jnp.exp(draws), dims[position] // shards_of).reshape((-1,) + (1,) * (len(dims) - 1 - position))
    return loudness


def scatter_about(own_key, extent, deviation, most, split=(), held_as=jnp.bfloat16):
    factor_of = level_of(own_key, extent, split, -0.22, 0.18) if split else 1.0
    entries = jax.random.normal(own_key, extent, jnp.float32) * deviation * factor_of
    return jnp.minimum(jnp.maximum(entries, -most), most).astype(held_as)


def setup_inputs(seed: int = 0) -> dict:
    streams_of = jax.random.split(jax.random.key(seed), 6)
    left = scatter_about(streams_of[0], (S, C, R), 1.0, 6.0, ((0, 16), (2, 16)))
    right = scatter_about(streams_of[1], (S, C, R), 1.0, 6.0, ((0, 16), (2, 16)))
    out_weight = scatter_about(streams_of[2], (C * C, K), (C * C // S) ** -0.5, 1.0)
    out_bias = scatter_about(streams_of[3], (K,), 0.5, 3.0, (), jnp.float32)
    cotangent = scatter_about(streams_of[4], (R, R, K), 0.0625, 0.5, ((0, 16), (1, 16)))
    return {"left": left, "right": right, "out_weight": out_weight, "out_bias": out_bias, "cotangent": cotangent}


def reference(left, right, out_weight, out_bias, cotangent):
    residues = left.shape[2]
    rows_per_block = math.gcd(16, residues)
    total_block_count = residues // rows_per_block
    left_wide = left.astype(jnp.float32)
    right_wide = right.astype(jnp.float32)
    bias_wide = out_bias.astype(jnp.float32)

    def block_step(running, block_index):
        start = (block_index * rows_per_block).astype(jnp.int32)
        left_block = lax.dynamic_slice_in_dim(left_wide, start, rows_per_block, 2)
        outer_sum = jnp.einsum("sci,sej->ijce", left_block, right_wide) / S
        outer_flat = outer_sum.astype(jnp.bfloat16).reshape(rows_per_block * residues, C * C)
        pair_out = jnp.dot(outer_flat, out_weight, preferred_element_type=jnp.float32) + bias_wide
        pair_out = pair_out.astype(jnp.bfloat16).reshape(rows_per_block, residues, K)
        cot_block = lax.dynamic_slice_in_dim(cotangent, start, rows_per_block, 0).reshape(rows_per_block * residues, K)
        d_outer = lax.dot_general(cot_block, out_weight, (((1,), (1,)), ((), ())), preferred_element_type=jnp.float32)
        d_outer = d_outer.astype(jnp.bfloat16).reshape(rows_per_block, residues, C, C).astype(jnp.float32)
        grad_block = jnp.einsum("ijce,sej->sci", d_outer, right_wide) / S
        running = running + jnp.einsum("ijce,sci->sej", d_outer, left_block) / S
        return running, (pair_out, grad_block)

    starting_value = jnp.zeros((S, C, residues), jnp.float32)
    grad_right, (pairs, grad_blocks) = lax.scan(block_step, starting_value, jnp.arange(total_block_count, dtype=jnp.int32))
    pair_update = pairs.reshape(residues, residues, K)
    grad_left = jnp.transpose(grad_blocks, (1, 2, 0, 3)).reshape(S, C, residues)
    return pair_update, grad_left, grad_right
```

```python
import functools

import jax
import jax.numpy as jnp
from jax import lax
from jax.experimental import pallas as pl
from jax.experimental.pallas import tpu as pltpu
from jax.sharding import PartitionSpec as P

F32 = jnp.float32
BF16 = jnp.bfloat16
MESH = pl.DeviceIdType.MESH

N = 16
S = 32
C = 32
K = 128
T = 128
H = S // 2
IC = 16
IB = 8
NEAR = ((0, 1), (1, 0), (1, 1), (3, 0), (3, 1), (2, 0), (2, 1))
ALL_YC = ((0, 0), (0, 1), (1, 0), (1, 1), (3, 0), (3, 1), (2, 0), (2, 1))


def owner(h, half):
    return 4 * (h // 2) + 2 * half + h % 2


def greet(barrier, me_w, me_n):
    for d in range(1, N):
        pl.semaphore_signal(
            barrier, inc=1, device_id={"wide": (me_w + d) % N}, device_id_type=MESH
        )
        pl.semaphore_signal(
            barrier, inc=1, device_id={"narrow": (me_n + d) % N}, device_id_type=MESH
        )


def cot_copies(cot_hbm, cot_buf, sems):
    return [
        pltpu.make_async_copy(
            cot_hbm.at[pl.ds(t * IC, IC)], cot_buf.at[pl.ds(t * IC, IC)], sems.at[t]
        )
        for t in range(T // IC)
    ]


def left_gradient_half(rows_ref, w2t_ref, cot_hbm, cot_buf, cot_sem, spread, sums):
    def step(t, _):
        base = pl.multiple_of(t * IC, IC)
        pltpu.make_async_copy(
            cot_hbm.at[pl.ds(base, IC)], cot_buf.at[pl.ds(base, IC)], cot_sem.at[t]
        ).wait()
        for p in range(IC // 2):
            pair = jnp.concatenate([cot_buf[base + 2 * p], cot_buf[base + 2 * p + 1]], axis=1)
            g = jnp.dot(rows_ref[...], pair, preferred_element_type=F32).astype(BF16)
            for q in range(2):
                r = (2 * p + q) * H
                for e in range(C):
                    spread[r : r + H, e * K : (e + 1) * K] = g[
                        e * H : (e + 1) * H, q * K : (q + 1) * K
                    ]
        out = jnp.dot(spread[...], w2t_ref[...], preferred_element_type=F32)
        sums[pl.ds(pl.multiple_of(t * IC * H, IC * H), IC * H), 0:C] = out * (1.0 / S)
        return 0

    lax.fori_loop(0, T // IC, step, 0)


def blocks_of(sums, blocks):
    for s in range(H):
        mine = sums[pl.ds(s, T, stride=H), :]
        blocks[s // 2, (s % 2) * C : (s % 2 + 1) * C, :] = mine.T[0:C, :].astype(BF16)


def gather_kernel(
    left_ref, right_ref, w_ref, cot_hbm,
    lt_ref, rt_ref, rb_ref, w2_ref, w2t_ref, first_ref,
    l_buf, r_buf, cot_buf, wide_f, rows_a, lt_f, spread, sums,
    cot_sem, lsend, lrecv, rsend, rrecv,
):
    me_w = lax.axis_index("wide")
    me_n = lax.axis_index("narrow")
    x_hi = (me_w // 2) % 2
    y = me_w // 4
    core = me_w % 2
    barrier = pltpu.get_barrier_semaphore()
    greet(barrier, me_w, me_n)
    for copy in cot_copies(cot_hbm, cot_buf, cot_sem):
        copy.start()

    wide_f[...] = w_ref[...].astype(F32)
    for e in range(C):
        part = wide_f[pl.ds(e, C, stride=C), :]
        w2_ref[:, e * K : (e + 1) * K] = part.astype(BF16)
        w2t_ref[e * K : (e + 1) * K, :] = part.T.astype(BF16)

    pl.semaphore_wait(barrier, 2 * (N - 1))

    def right_copy(dy, dx, dc):
        to = ((y + dy) % 4) * 4 + ((x_hi + dx) % 2) * 2 + (core + dc) % 2
        k = dy * 4 + dx * 2 + dc
        return pltpu.make_async_remote_copy(
            right_ref, r_buf.at[me_w], rsend.at[k], rrecv.at[me_w],
            device_id={"wide": to}, device_id_type=MESH,
        )

    def left_copy(d):
        return pltpu.make_async_remote_copy(
            left_ref, l_buf.at[me_n], lsend.at[d], lrecv.at[me_n],
            device_id={"narrow": (me_n + d) % N}, device_id_type=MESH,
        )

    sends = [right_copy(dy, 0, dc) for dy, dc in NEAR]
    sends += [left_copy(d) for d in (1, 15, 8, 2, 14, 9, 7, 3, 13, 10, 6, 4, 12, 11, 5)]
    sends += [right_copy(dy, 1, dc) for dy, dc in ALL_YC]
    for copy in sends:
        copy.start()
    r_buf[me_w] = right_ref[...]
    l_buf[me_n] = left_ref[...]

    def right_arrived(w):
        pltpu.make_async_remote_copy(
            right_ref, r_buf.at[w], rsend.at[0], rrecv.at[w],
            device_id={"wide": w}, device_id_type=MESH,
        ).wait_recv()

    def left_arrived(n):
        pltpu.make_async_remote_copy(
            left_ref, l_buf.at[n], lsend.at[0], lrecv.at[n],
            device_id={"narrow": n}, device_id_type=MESH,
        ).wait_recv()

    for dy, dc in NEAR:
        right_arrived(((y + dy) % 4) * 4 + x_hi * 2 + (core + dc) % 2)
    for h in range(8):
        wide_f[h * 64 : (h + 1) * 64, :] = r_buf[owner(h, x_hi)].astype(F32)
    for e in range(C):
        rows_a[e * H : (e + 1) * H, :] = wide_f[pl.ds(e, H, stride=C), :].astype(BF16)

    left_gradient_half(rows_a, w2t_ref, cot_hbm, cot_buf, cot_sem, spread, sums)
    blocks_of(sums, first_ref)

    for dy, dc in ALL_YC:
        right_arrived(((y + dy) % 4) * 4 + (1 - x_hi) * 2 + (core + dc) % 2)
    for h in range(8):
        wide_f[h * 64 : (h + 1) * 64, :] = r_buf[owner(h, 1 - x_hi)].astype(F32)
    for e in range(C):
        rb_ref[e * H : (e + 1) * H, :] = wide_f[pl.ds(e, H, stride=C), :].astype(BF16)
    for w in range(N):
        wide_f[w * 64 : (w + 1) * 64, :] = r_buf[w].astype(F32)
    for b in range(8):
        rows = jnp.concatenate(
            [wide_f[pl.ds(4 * b + q, S, stride=C), :] for q in range(4)], axis=0
        )
        rt_ref[:, b * 128 : (b + 1) * 128] = rows.T.astype(BF16)
    for d in range(1, N):
        left_arrived((me_n + d) % N)
    for n in range(N):
        for q in range(2):
            part = l_buf[n, q * C : (q + 1) * C, :].astype(F32) * (1.0 / S)
            lt_f[pl.ds(2 * n + q, T, stride=S), 0:C] = part.T
    lt_ref[...] = lt_f[:, 0:C].astype(BF16)
    for copy in sends:
        copy.wait_send()


def gather(left, right, weight, cot):
    vmem = pl.BlockSpec(memory_space=pltpu.VMEM)
    return pl.pallas_call(
        gather_kernel,
        out_shape=(
            jax.ShapeDtypeStruct((T * S, C), BF16),
            jax.ShapeDtypeStruct((T, C * S), BF16),
            jax.ShapeDtypeStruct((C * H, T), BF16),
            jax.ShapeDtypeStruct((C, C * K), BF16),
            jax.ShapeDtypeStruct((C * K, C), BF16),
            jax.ShapeDtypeStruct((8, 64, T), BF16),
        ),
        in_specs=[vmem, vmem, vmem, pl.BlockSpec(memory_space=pl.ANY)],
        out_specs=(vmem,) * 6,
        scratch_shapes=[
            pltpu.VMEM((N, 64, T), BF16),
            pltpu.VMEM((N, 64, T), BF16),
            pltpu.VMEM((T, T, K), BF16),
            pltpu.VMEM((C * S, 128), F32),
            pltpu.VMEM((C * H, T), BF16),
            pltpu.VMEM((T * S, 128), F32),
            pltpu.VMEM((IC * H, C * K), BF16),
            pltpu.VMEM((T * H, 128), F32),
            pltpu.SemaphoreType.DMA((T // IC,)),
            pltpu.SemaphoreType.DMA((N,)),
            pltpu.SemaphoreType.DMA((N,)),
            pltpu.SemaphoreType.DMA((N,)),
            pltpu.SemaphoreType.DMA((N,)),
        ],
        compiler_params=pltpu.CompilerParams(
            collective_id=0, has_side_effects=True, vmem_limit_bytes=48 << 20
        ),
        name="gather_kernel",
    )(left, right, weight, cot)


def pair_kernel(lt_ref, rt_ref, w2_ref, bias_ref, cot_ref, pair_ref, dr_ref, t_buf, acc):
    g = pl.program_id(0)

    @pl.when(g == 0)
    def _():
        acc[...] = jnp.zeros_like(acc)

    lt = lt_ref[...]
    for b in range(C // 2):
        t = jnp.dot(lt, w2_ref[:, b * 256 : (b + 1) * 256], preferred_element_type=F32)
        t = t.astype(BF16)
        for i in range(IB):
            for q in range(2):
                e = 2 * b + q
                t_buf[e * S : (e + 1) * S, i * K : (i + 1) * K] = t[
                    i * S : (i + 1) * S, q * K : (q + 1) * K
                ]
    out = jnp.dot(rt_ref[...], t_buf[...], preferred_element_type=F32)
    for i in range(IB):
        pair_ref[i] = (out[:, i * K : (i + 1) * K] + bias_ref[...]).astype(BF16)
    cot = jnp.concatenate([cot_ref[i] for i in range(IB)], axis=1)
    acc[...] += lax.dot_general(
        t_buf[...], cot, (((1,), (1,)), ((), ())), preferred_element_type=F32
    )

    @pl.when(g == pl.num_programs(0) - 1)
    def _():
        for s in range(S):
            dr_ref[s // 2, (s % 2) * C : (s % 2 + 1) * C, :] = acc[
                pl.ds(s, C, stride=S), :
            ].astype(BF16)


def pairs(lt, rt, w2, bias, cot):
    whole = lambda shape: pl.BlockSpec(shape, lambda g: (0,) * len(shape))
    return pl.pallas_call(
        pair_kernel,
        grid=(T // IB,),
        out_shape=(
            jax.ShapeDtypeStruct((T, T, K), BF16),
            jax.ShapeDtypeStruct((N, 64, T), BF16),
        ),
        in_specs=[
            pl.BlockSpec((IB * S, C), lambda g: (g, 0)),
            whole((T, C * S)),
            whole((C, C * K)),
            whole((1, K)),
            pl.BlockSpec((IB, T, K), lambda g: (g, 0, 0)),
        ],
        out_specs=(pl.BlockSpec((IB, T, K), lambda g: (g, 0, 0)), whole((N, 64, T))),
        scratch_shapes=[pltpu.VMEM((C * S, IB * K), BF16), pltpu.VMEM((C * S, T), F32)],
        compiler_params=pltpu.CompilerParams(
            dimension_semantics=("arbitrary",), vmem_limit_bytes=48 << 20
        ),
        name="pair_kernel",
    )(lt, rt, w2, bias, cot)


def scatter_kernel(
    dr_ref, first_ref, rb_ref, w2t_ref, cot_hbm,
    gl_ref, gr_ref,
    dr_in, dl_in, second, cot_buf, spread, sums,
    cot_sem, rsend, rrecv, lsend, lrecv,
):
    me_w = lax.axis_index("wide")
    me_n = lax.axis_index("narrow")
    x_hi = (me_w // 2) % 2
    barrier = pltpu.get_barrier_semaphore()
    greet(barrier, me_w, me_n)
    for copy in cot_copies(cot_hbm, cot_buf, cot_sem):
        copy.start()
    pl.semaphore_wait(barrier, 2 * (N - 1))

    def right_copy(d):
        to = (me_w + d) % N
        return pltpu.make_async_remote_copy(
            dr_ref.at[to], dr_in.at[me_w], rsend.at[d], rrecv.at[me_w],
            device_id={"wide": to}, device_id_type=MESH,
        )

    def left_copy(blocks, h, half):
        to = owner(h, half)
        return pltpu.make_async_remote_copy(
            blocks.at[h], dl_in.at[me_n], lsend.at[to], lrecv.at[me_n],
            device_id={"narrow": to}, device_id_type=MESH,
        )

    for d in range(1, N):
        right_copy(d).start()
    for h in range(8):
        @pl.when(owner(h, x_hi) != me_n)
        def _():
            left_copy(first_ref, h, x_hi).start()

    left_gradient_half(rb_ref, w2t_ref, cot_hbm, cot_buf, cot_sem, spread, sums)
    blocks_of(sums, second)
    for h in range(8):
        @pl.when(owner(h, 1 - x_hi) != me_n)
        def _():
            left_copy(second, h, 1 - x_hi).start()

    for h in range(8):
        @pl.when(owner(h, x_hi) == me_n)
        def _():
            dl_in[me_n] = first_ref[h]

        @pl.when(owner(h, 1 - x_hi) == me_n)
        def _():
            dl_in[me_n] = second[h]

    dr_in[me_w] = dr_ref[me_w]
    for d in range(1, N):
        w = (me_w + d) % N
        pltpu.make_async_remote_copy(
            dr_ref.at[w], dr_in.at[w], rsend.at[d], rrecv.at[w],
            device_id={"wide": w}, device_id_type=MESH,
        ).wait_recv()
    total = dr_in[0].astype(F32)
    for w in range(1, N):
        total += dr_in[w].astype(F32)
    gr_ref[...] = total
    for d in range(1, N):
        n = (me_n + d) % N
        pltpu.make_async_remote_copy(
            second.at[0], dl_in.at[n], lsend.at[n], lrecv.at[n],
            device_id={"narrow": n}, device_id_type=MESH,
        ).wait_recv()
    total = dl_in[0].astype(F32)
    for n in range(1, N):
        total += dl_in[n].astype(F32)
    gl_ref[...] = total
    for d in range(1, N):
        right_copy(d).wait_send()
    for h in range(8):
        @pl.when(owner(h, x_hi) != me_n)
        def _():
            left_copy(first_ref, h, x_hi).wait_send()

        @pl.when(owner(h, 1 - x_hi) != me_n)
        def _():
            left_copy(second, h, 1 - x_hi).wait_send()


def scatter(dr, first, rb, w2t, cot):
    vmem = pl.BlockSpec(memory_space=pltpu.VMEM)
    return pl.pallas_call(
        scatter_kernel,
        out_shape=(
            jax.ShapeDtypeStruct((64, T), F32),
            jax.ShapeDtypeStruct((64, T), F32),
        ),
        in_specs=[vmem] * 4 + [pl.BlockSpec(memory_space=pl.ANY)],
        out_specs=(vmem, vmem),
        scratch_shapes=[
            pltpu.VMEM((N, 64, T), BF16),
            pltpu.VMEM((N, 64, T), BF16),
            pltpu.VMEM((8, 64, T), BF16),
            pltpu.VMEM((T, T, K), BF16),
            pltpu.VMEM((IC * H, C * K), BF16),
            pltpu.VMEM((T * H, 128), F32),
            pltpu.SemaphoreType.DMA((T // IC,)),
            pltpu.SemaphoreType.DMA((N,)),
            pltpu.SemaphoreType.DMA((N,)),
            pltpu.SemaphoreType.DMA((N,)),
            pltpu.SemaphoreType.DMA((N,)),
        ],
        compiler_params=pltpu.CompilerParams(
            collective_id=1, has_side_effects=True, vmem_limit_bytes=48 << 20
        ),
        name="scatter_kernel",
    )(dr, first, rb, w2t, cot)


def local(left, right, out_weight, out_bias, cotangent):
    lt, rt, rb, w2, w2t, first = gather(
        left.reshape(64, T), right.reshape(64, T), out_weight, cotangent
    )
    pair_update, dr = pairs(lt, rt, w2, out_bias.reshape(1, K), cotangent)
    gl, gr = scatter(dr, first, rb, w2t, cotangent)
    return pair_update, gl.reshape(2, C, T), gr.reshape(2, C, T)


def solution(mesh):
    return jax.shard_map(
        local,
        mesh=mesh,
        in_specs=(
            P("narrow", None, "wide"),
            P("wide", None, "narrow"),
            P(),
            P(),
            P("wide", "narrow", None),
        ),
        out_specs=(P("wide", "narrow", None), P("narrow", None, "wide"), P("wide", None, "narrow")),
        check_vma=False,
    )
```

```python
import jax
import jax.numpy as jnp
from jax import lax
from jax.experimental import pallas as pl
from jax.experimental.pallas import tpu as pltpu
from jax.sharding import PartitionSpec as P

F32 = jnp.float32
BF16 = jnp.bfloat16
MESH = pl.DeviceIdType.MESH
NT = (((1,), (1,)), ((), ()))

N = 16
S = 32
C = 32
K = 128
T = 128
HALF = T // 2
IC = 16
IM = 16
IB = 8
NEAR_FIRST = (1, 15, 8, 2, 14, 9, 7, 3, 13, 10, 6, 4, 12, 11, 5)


def greet(barrier, me_w, me_n):
    for d in range(1, N):
        pl.semaphore_signal(
            barrier, inc=1, device_id={"wide": (me_w + d) % N}, device_id_type=MESH
        )
        pl.semaphore_signal(
            barrier, inc=1, device_id={"narrow": (me_n + d) % N}, device_id_type=MESH
        )


def push(axis, me, d, src, dst, send_sem, recv_sem):
    return pltpu.make_async_remote_copy(
        src, dst.at[me], send_sem.at[d], recv_sem.at[me],
        device_id={axis: (me + d) % N}, device_id_type=MESH,
    )


def arrived(axis, me, d, src, dst, send_sem, recv_sem):
    peer = (me + d) % N
    pltpu.make_async_remote_copy(
        src, dst.at[peer], send_sem.at[d], recv_sem.at[peer],
        device_id={axis: peer}, device_id_type=MESH,
    ).wait_recv()


def cot_copy(cot_hbm, cot_buf, sems, first, t):
    at = pl.multiple_of(t * IC, IC)
    return pltpu.make_async_copy(
        cot_hbm.at[pl.ds(first + at, IC)], cot_buf.at[pl.ds(at, IC)], sems.at[t]
    )


def project_cotangent(first, steps, wec_ref, cot_hbm, cot_buf, cot_sem, spread):
    def step(t, _):
        cot_copy(cot_hbm, cot_buf, cot_sem, first, t).wait()
        base = t * IC
        for p in range(IC // 2):
            rows = cot_buf[pl.ds(base + 2 * p, 2)].reshape(2 * T, K)
            d = lax.dot_general(wec_ref[...], rows, NT, preferred_element_type=F32)
            d = d.astype(BF16)
            for q in range(2):
                for e in range(C):
                    spread[base + 2 * p + q, e] = d[e * C : (e + 1) * C, q * T : (q + 1) * T]
        return 0

    lax.fori_loop(steps[0], steps[1], step, 0)


def left_gradient(spread, rmat_ref, sums, beside):
    def step(t, _):
        at = pl.multiple_of(t * IM * C, IM * C)
        rows = jnp.concatenate(
            [spread[pl.ds(t * IM, IM), e].reshape(IM * C, T) for e in range(C)], axis=1
        )
        out = jnp.dot(rows, rmat_ref[...], preferred_element_type=F32)
        sums[pl.ds(at, IM * C), 0:S] = out * (1.0 / S)
        beside(t)
        return 0

    lax.fori_loop(0, HALF // IM, step, 0)


def blocks_of(sums, turned, blocks):
    for c in range(C):
        part = sums[pl.ds(c, HALF, stride=C), :].T
        turned[c * N : (c + 1) * N, :] = jnp.concatenate([part[0:N], part[N : 2 * N]], axis=1)
    for n in range(N):
        blocks[n] = turned[pl.ds(n, C, stride=N), :].astype(BF16)


def gather_kernel(
    left_hbm, right_hbm, w_hbm, cot_hbm,
    lt_ref, rt_ref, w2_ref, wec_ref, rmat_ref, first_ref,
    left_v, right_v, w_v, l_buf, r_buf, cot_buf, wide_f, left_f, lt_f, spread, sums, turned,
    in_sem, cot_sem, lsend, lrecv, rsend, rrecv,
):
    me_w = lax.axis_index("wide")
    me_n = lax.axis_index("narrow")
    barrier = pltpu.get_barrier_semaphore()
    fetch_w = pltpu.make_async_copy(w_hbm, w_v, in_sem.at[0])
    fetch_l = pltpu.make_async_copy(left_hbm, left_v, in_sem.at[1])
    fetch_r = pltpu.make_async_copy(right_hbm, right_v, in_sem.at[2])
    fetch_w.start()
    fetch_l.start()
    fetch_r.start()
    for t in range(HALF // IC):
        cot_copy(cot_hbm, cot_buf, cot_sem, 0, t).start()
    greet(barrier, me_w, me_n)

    fetch_w.wait()
    wide_f[...] = w_v[...].astype(F32)
    for e in range(C):
        part = wide_f[pl.ds(e, C, stride=C), :].astype(BF16)
        w2_ref[e] = part
        wec_ref[e * C : (e + 1) * C, :] = part
    fetch_l.wait()
    fetch_r.wait()

    project_cotangent(0, (0, AHEAD), wec_ref, cot_hbm, cot_buf, cot_sem, spread)
    pl.semaphore_wait(barrier, 2 * (N - 1))
    sends = [
        push("wide", me_w, d, right_v, r_buf, rsend, rrecv) for d in NEAR_FIRST
    ]
    sends += [
        push("narrow", me_n, d, left_v, l_buf, lsend, lrecv) for d in NEAR_FIRST
    ]
    for copy in sends:
        copy.start()
    project_cotangent(0, (AHEAD, HALF // IC), wec_ref, cot_hbm, cot_buf, cot_sem, spread)

    r_buf[me_w] = right_v[...]
    l_buf[me_n] = left_v[...]
    for d in range(1, N):
        arrived("wide", me_w, d, right_v, r_buf, rsend, rrecv)
    for w in range(N):
        wide_f[w * 64 : (w + 1) * 64, :] = r_buf[w].astype(F32)
    for e in range(C):
        rows = jnp.concatenate(
            [wide_f[pl.ds(q * C + e, N, stride=2 * C), :] for q in range(2)], axis=0
        )
        rmat_ref[e * T : (e + 1) * T, :] = rows.T.astype(BF16)
    for d in range(1, N):
        arrived("narrow", me_n, d, left_v, l_buf, lsend, lrecv)
    for n in range(N):
        left_f[n * 64 : (n + 1) * 64, :] = l_buf[n].astype(F32) * (1.0 / S)

    def beside(t):
        for b in range(2):
            rows = jnp.concatenate(
                [wide_f[pl.ds(8 * t + 4 * b + q, S, stride=C), :] for q in range(4)], axis=0
            )
            rt_ref[2 * t + b] = rows.T.astype(BF16)
        for q in range(8):
            s = 8 * t + q
            part = left_f[pl.ds(pl.multiple_of(s * C, C), C), :]
            lt_f[pl.ds(s, T, stride=S), 0:C] = part.T

    left_gradient(spread, rmat_ref, sums, beside)
    lt_ref[...] = lt_f[:, 0:C].astype(BF16)
    blocks_of(sums, turned, first_ref)
    for copy in sends:
        copy.wait_send()


def gather(left, right, weight, cot):
    vmem = pl.BlockSpec(memory_space=pltpu.VMEM)
    hbm = pl.BlockSpec(memory_space=pltpu.HBM)
    return pl.pallas_call(
        gather_kernel,
        out_shape=(
            jax.ShapeDtypeStruct((T * S, C), BF16),
            jax.ShapeDtypeStruct((C // 4, T, 4 * S), BF16),
            jax.ShapeDtypeStruct((C, C, K), BF16),
            jax.ShapeDtypeStruct((C * C, K), BF16),
            jax.ShapeDtypeStruct((C * T, S), BF16),
            jax.ShapeDtypeStruct((N, C, T), BF16),
        ),
        in_specs=[hbm] * 4,
        out_specs=(vmem,) * 6,
        scratch_shapes=[
            pltpu.VMEM((64, T), BF16),
            pltpu.VMEM((64, T), BF16),
            pltpu.VMEM((C * C, K), BF16),
            pltpu.VMEM((N, 64, T), BF16),
            pltpu.VMEM((N, 64, T), BF16),
            pltpu.VMEM((HALF, T, K), BF16),
            pltpu.VMEM((C * S, 128), F32),
            pltpu.VMEM((C * S, 128), F32),
            pltpu.VMEM((T * S, 128), F32),
            pltpu.VMEM((HALF, C, C, T), BF16),
            pltpu.VMEM((HALF * C, 128), F32),
            pltpu.VMEM((C * N, 128), F32),
            pltpu.SemaphoreType.DMA((3,)),
            pltpu.SemaphoreType.DMA((HALF // IC,)),
            pltpu.SemaphoreType.DMA((N,)),
            pltpu.SemaphoreType.DMA((N,)),
            pltpu.SemaphoreType.DMA((N,)),
            pltpu.SemaphoreType.DMA((N,)),
        ],
        compiler_params=pltpu.CompilerParams(
            collective_id=0, has_side_effects=True, vmem_limit_bytes=40 << 20
        ),
        name="gather_kernel",
    )(*[pltpu.with_memory_space_constraint(x, pltpu.HBM) for x in (left, right, weight, cot)])


AHEAD = 2


def intermediate_tile(lt, w2_ref, t_buf, b):
    w = jnp.concatenate([w2_ref[2 * b], w2_ref[2 * b + 1]], axis=1)
    t = jnp.dot(lt, w, preferred_element_type=F32).astype(BF16)
    for i in range(IB):
        for q in range(2):
            e = 2 * b + q
            t_buf[i, e * S : (e + 1) * S, :] = t[i * S : (i + 1) * S, q * K : (q + 1) * K]


def pair_kernel(lt_ref, rt_ref, w2_ref, bias_ref, cot_ref, pair_ref, dr_ref, t_a, t_b, acc_t, acc):
    g = pl.program_id(0)

    def lt_of(chunk):
        at = jnp.minimum(chunk, T // IB - 1) * (IB * S)
        return lt_ref[pl.ds(pl.multiple_of(at, IB * S), IB * S), :]

    @pl.when(g == 0)
    def _():
        acc_t[...] = jnp.zeros_like(acc_t)
        lt = lt_of(0)
        for b in range(C // 2):
            intermediate_tile(lt, w2_ref, t_a, b)

    for half, (now, later) in enumerate(((t_a, t_b), (t_b, t_a))):
        lt = lt_of(2 * g + half + 1)
        first = half * IB
        cot = jnp.concatenate([cot_ref[first + i] for i in range(IB)], axis=1)

        def pair_of(p):
            rows = jnp.concatenate([rt_ref[b] for b in range(C // 4)], axis=1)
            both = jnp.concatenate([now[2 * p], now[2 * p + 1]], axis=1)
            out = jnp.dot(rows, both, preferred_element_type=F32)
            for q in range(2):
                pair_ref[first + 2 * p + q] = (
                    out[:, q * K : (q + 1) * K] + bias_ref[...]
                ).astype(BF16)

        def right_of(n):
            turned = jnp.concatenate(
                [
                    jnp.concatenate(
                        [
                            now[i, n * 256 + a * 128 : n * 256 + (a + 1) * 128, :].T
                            for a in range(2)
                        ],
                        axis=1,
                    )
                    for i in range(IB)
                ],
                axis=0,
            )
            acc_t[:, n * 256 : (n + 1) * 256] += jnp.dot(
                cot, turned, preferred_element_type=F32
            )

        for n in range(4):
            for b in range(4 * n, 4 * n + 2):
                intermediate_tile(lt, w2_ref, later, b)
            right_of(n)
            for b in range(4 * n + 2, 4 * n + 4):
                intermediate_tile(lt, w2_ref, later, b)
            pair_of(n)

    @pl.when(g == pl.num_programs(0) - 1)
    def _():
        for b in range(8):
            acc[b * 128 : (b + 1) * 128, :] = acc_t[:, b * 128 : (b + 1) * 128].T
        for s in range(S):
            dr_ref[s // 2, (s % 2) * C : (s % 2 + 1) * C, :] = acc[
                pl.ds(s, C, stride=S), :
            ].astype(BF16)


def pairs(lt, rt, w2, bias, cot):
    whole = lambda shape: pl.BlockSpec(shape, lambda g: (0,) * len(shape))
    step = pl.BlockSpec((2 * IB, T, K), lambda g: (g, 0, 0))
    return pl.pallas_call(
        pair_kernel,
        grid=(T // (2 * IB),),
        out_shape=(
            jax.ShapeDtypeStruct((T, T, K), BF16),
            jax.ShapeDtypeStruct((N, 64, T), BF16),
        ),
        in_specs=[
            whole((T * S, C)),
            whole((C // 4, T, 4 * S)),
            whole((C, C, K)),
            whole((1, K)),
            step,
        ],
        out_specs=(step, whole((N, 64, T))),
        scratch_shapes=[
            pltpu.VMEM((IB, C * S, K), BF16),
            pltpu.VMEM((IB, C * S, K), BF16),
            pltpu.VMEM((T, C * S), F32),
            pltpu.VMEM((C * S, T), F32),
        ],
        compiler_params=pltpu.CompilerParams(
            dimension_semantics=("arbitrary",), vmem_limit_bytes=40 << 20
        ),
        name="pair_kernel",
    )(lt, rt, w2, bias, cot)


def total_of(blocks):
    total = blocks[0].astype(F32)
    for n in range(1, N):
        total += blocks[n].astype(F32)
    return total


def scatter_kernel(
    dr_ref, first_ref, wec_ref, rmat_ref, cot_hbm,
    gl_ref, gr_ref,
    dr_in, dl_in, dm_in, second, cot_buf, spread, sums, turned,
    cot_sem, rsend, rrecv, lsend, lrecv, msend, mrecv,
):
    me_w = lax.axis_index("wide")
    me_n = lax.axis_index("narrow")
    barrier = pltpu.get_barrier_semaphore()
    for t in range(HALF // IC):
        cot_copy(cot_hbm, cot_buf, cot_sem, HALF, t).start()
    greet(barrier, me_w, me_n)
    project_cotangent(HALF, (0, AHEAD), wec_ref, cot_hbm, cot_buf, cot_sem, spread)
    pl.semaphore_wait(barrier, 2 * (N - 1))

    def piece(blocks, me, d):
        return blocks.at[(me + d) % N]

    sends = [
        push("wide", me_w, d, piece(dr_ref, me_w, d), dr_in, rsend, rrecv) for d in NEAR_FIRST
    ]
    sends += [
        push("narrow", me_n, d, piece(first_ref, me_n, d), dl_in, lsend, lrecv)
        for d in NEAR_FIRST
    ]
    for copy in sends:
        copy.start()
    dr_in[me_w] = dr_ref[me_w]
    dl_in[me_n] = first_ref[me_n]

    project_cotangent(HALF, (AHEAD, HALF // IC), wec_ref, cot_hbm, cot_buf, cot_sem, spread)
    left_gradient(spread, rmat_ref, sums, lambda t: None)
    blocks_of(sums, turned, second)
    last = [
        push("narrow", me_n, d, piece(second, me_n, d), dm_in, msend, mrecv)
        for d in NEAR_FIRST[::-1]
    ]
    for copy in last:
        copy.start()
    dm_in[me_n] = second[me_n]

    for d in range(1, N):
        arrived("wide", me_w, d, piece(dr_ref, me_w, d), dr_in, rsend, rrecv)
    gr_ref[...] = total_of(dr_in)
    for d in range(1, N):
        arrived("narrow", me_n, d, piece(first_ref, me_n, d), dl_in, lsend, lrecv)
    one = total_of(dl_in)
    for copy in sends:
        copy.wait_send()
    for d in range(1, N):
        arrived("narrow", me_n, d, piece(second, me_n, d), dm_in, msend, mrecv)
    two = total_of(dm_in)
    for q in range(2):
        gl_ref[q * C : (q + 1) * C, :] = jnp.concatenate(
            [part[:, q * HALF : (q + 1) * HALF] for part in (one, two)], axis=1
        )
    for copy in last:
        copy.wait_send()


def scatter(dr, first, wec, rmat, cot):
    vmem = pl.BlockSpec(memory_space=pltpu.VMEM)
    return pl.pallas_call(
        scatter_kernel,
        out_shape=(
            jax.ShapeDtypeStruct((64, T), F32),
            jax.ShapeDtypeStruct((64, T), F32),
        ),
        in_specs=[vmem] * 4 + [pl.BlockSpec(memory_space=pltpu.HBM)],
        out_specs=(vmem, vmem),
        scratch_shapes=[
            pltpu.VMEM((N, 64, T), BF16),
            pltpu.VMEM((N, C, T), BF16),
            pltpu.VMEM((N, C, T), BF16),
            pltpu.VMEM((N, C, T), BF16),
            pltpu.VMEM((HALF, T, K), BF16),
            pltpu.VMEM((HALF, C, C, T), BF16),
            pltpu.VMEM((HALF * C, 128), F32),
            pltpu.VMEM((C * N, 128), F32),
            pltpu.SemaphoreType.DMA((HALF // IC,)),
        ]
        + [pltpu.SemaphoreType.DMA((N,))] * 6,
        compiler_params=pltpu.CompilerParams(
            collective_id=1, has_side_effects=True, vmem_limit_bytes=40 << 20
        ),
        name="scatter_kernel",
    )(dr, first, wec, rmat, pltpu.with_memory_space_constraint(cot, pltpu.HBM))


def local(left, right, out_weight, out_bias, cotangent):
    lt, rt, w2, wec, rmat, first = gather(
        left.reshape(64, T), right.reshape(64, T), out_weight, cotangent
    )
    pair_update, dr = pairs(lt, rt, w2, out_bias.reshape(1, K), cotangent)
    gl, gr = scatter(dr, first, wec, rmat, cotangent)
    return pair_update, gl.reshape(2, C, T), gr.reshape(2, C, T)


def solution(mesh):
    return jax.shard_map(
        local,
        mesh=mesh,
        in_specs=(
            P("narrow", None, "wide"),
            P("wide", None, "narrow"),
            P(),
            P(),
            P("wide", "narrow", None),
        ),
        out_specs=(P("wide", "narrow", None), P("narrow", None, "wide"), P("wide", None, "narrow")),
        check_vma=False,
    )
```

```python
import jax
import jax.numpy as jnp
from jax import lax
from jax.experimental import pallas as pl
from jax.experimental.pallas import tpu as pltpu
from jax.sharding import PartitionSpec as P

F32 = jnp.float32
BF16 = jnp.bfloat16
MESH = pl.DeviceIdType.MESH
NT = (((1,), (1,)), ((), ()))

N = 16
S = 32
C = 32
K = 128
T = 128
IC = 16
IM = 16
IB = 8
IP = 16
AHEAD = 4
LATE = 2
NEAR_FIRST = (1, 15, 8, 2, 14, 9, 7, 3, 13, 10, 6, 4, 12, 11, 5)


def push(axis, me, d, src, dst, send_sem, recv_sem):
    return pltpu.make_async_remote_copy(
        src, dst.at[me], send_sem.at[d], recv_sem.at[me],
        device_id={axis: (me + d) % N}, device_id_type=MESH,
    )


def arrived(axis, me, d, src, dst, send_sem, recv_sem):
    peer = (me + d) % N
    pltpu.make_async_remote_copy(
        src, dst.at[peer], send_sem.at[d], recv_sem.at[peer],
        device_id={axis: peer}, device_id_type=MESH,
    ).wait_recv()


def cot_copy(cot_hbm, cot_buf, sems, t):
    at = pl.multiple_of(t * IC, IC)
    return pltpu.make_async_copy(
        cot_hbm.at[pl.ds(at, IC)], cot_buf.at[pl.ds(at, IC)], sems.at[t]
    )


def total_of(blocks):
    total = blocks[0].astype(F32)
    for n in range(1, N):
        total += blocks[n].astype(F32)
    return total


def kernel(
    left_hbm, right_hbm, w_hbm, bias_hbm, cot_hbm,
    pair_ref, gl_ref, gr_ref,
    left_v, right_v, w_v, bias_v, l_buf, r_buf, cot_buf, wide_f, left_f, lt_f, lt, rt, w2, wec, rmat,
    big, sums, turned, acc_t, dl_out, dr_out, dl_in, dr_in,
    in_sem, cot_sem, lsend, lrecv, rsend, rrecv, dlsend, dlrecv, drsend, drrecv,
):
    me_w = lax.axis_index("wide")
    me_n = lax.axis_index("narrow")
    barrier = pltpu.get_barrier_semaphore()
    for d in range(1, N):
        pl.semaphore_signal(
            barrier, inc=1, device_id={"wide": (me_w + d) % N}, device_id_type=MESH
        )
        pl.semaphore_signal(
            barrier, inc=1, device_id={"narrow": (me_n + d) % N}, device_id_type=MESH
        )
    fetches = [
        pltpu.make_async_copy(src, dst, in_sem.at[n])
        for n, (src, dst) in enumerate(
            ((w_hbm, w_v), (right_hbm, right_v), (left_hbm, left_v), (bias_hbm, bias_v))
        )
    ]
    for copy in fetches:
        copy.start()
    for t in range(T // IC):
        cot_copy(cot_hbm, cot_buf, cot_sem, t).start()

    fetches[0].wait()
    wide_f[...] = w_v[...].astype(F32)
    for e in range(C):
        part = wide_f[pl.ds(e, C, stride=C), :].astype(BF16)
        w2[e] = part
        wec[e * C : (e + 1) * C, :] = part
    for copy in fetches[1:]:
        copy.wait()

    def project(t, _):
        cot_copy(cot_hbm, cot_buf, cot_sem, t).wait()
        base = t * IC
        for p in range(IC // 2):
            rows = cot_buf[pl.ds(base + 2 * p, 2)].reshape(2 * T, K)
            d = lax.dot_general(wec[...], rows, NT, preferred_element_type=F32)
            d = d.astype(BF16)
            for q in range(2):
                big[base + 2 * p + q] = d[:, q * T : (q + 1) * T]
        return 0

    lax.fori_loop(0, AHEAD, project, 0)
    pl.semaphore_wait(barrier, 2 * (N - 1))
    sends = [push("wide", me_w, d, right_v, r_buf, rsend, rrecv) for d in NEAR_FIRST]
    sends += [push("narrow", me_n, d, left_v, l_buf, lsend, lrecv) for d in NEAR_FIRST]
    for copy in sends:
        copy.start()
    r_buf[me_w] = right_v[...]
    l_buf[me_n] = left_v[...]
    lax.fori_loop(AHEAD, T // IC, project, 0)

    for d in range(1, N):
        arrived("wide", me_w, d, right_v, r_buf, rsend, rrecv)
    for w in range(N):
        wide_f[w * 64 : (w + 1) * 64, :] = r_buf[w].astype(F32)
    for e in range(C):
        rmat[e * T : (e + 1) * T, :] = wide_f[pl.ds(e, S, stride=C), :].T.astype(BF16)

    def left_gradient(t):
        rows = jnp.concatenate(
            [
                big[pl.ds(t * IM, IM), e * C : (e + 1) * C, :].reshape(IM * C, T)
                for e in range(C)
            ],
            axis=1,
        )
        out = jnp.dot(rows, rmat[...], preferred_element_type=F32)
        sums[pl.ds(pl.multiple_of(t * IM * C, IM * C), IM * C), 0:S] = out * (1.0 / S)

    def early(t, _):
        left_gradient(t)
        return 0

    def late(t, _):
        left_gradient(t)
        u = t - (T // IM - LATE)
        for q in range(S // LATE):
            s = u * (S // LATE) + q
            part = left_f[pl.ds(pl.multiple_of(s * C, C), C), :]
            lt_f[pl.ds(s, T, stride=S), 0:C] = part.T
        for q in range(8 // LATE):
            b = u * (8 // LATE) + q
            rows = jnp.concatenate(
                [wide_f[pl.ds(4 * b + m, S, stride=C), :] for m in range(4)], axis=0
            )
            rt[b] = rows.T.astype(BF16)
        return 0

    lax.fori_loop(0, T // IM - LATE, early, 0)
    for d in range(1, N):
        arrived("narrow", me_n, d, left_v, l_buf, lsend, lrecv)
    for n in range(N):
        left_f[n * 64 : (n + 1) * 64, :] = l_buf[n].astype(F32) * (1.0 / S)
    lax.fori_loop(T // IM - LATE, T // IM, late, 0)
    lt[...] = lt_f[:, 0:C].astype(BF16)

    for c in range(C):
        turned[c * S : (c + 1) * S, :] = sums[pl.ds(c, T, stride=C), :].T[0:S]
    for s in range(S):
        dl_out[s // 2, (s % 2) * C : (s % 2 + 1) * C, :] = turned[
            pl.ds(s, C, stride=S), :
        ].astype(BF16)
    dl_sends = [
        push("narrow", me_n, d, dl_out.at[(me_n + d) % N], dl_in, dlsend, dlrecv)
        for d in NEAR_FIRST
    ]
    for copy in dl_sends:
        copy.start()
    dl_in[me_n] = dl_out[me_n]

    def intermediate(chunk, b):
        rows = lt[pl.ds(pl.multiple_of(chunk * (IB * S), IB * S), IB * S), :]
        w = jnp.concatenate([w2[2 * b], w2[2 * b + 1]], axis=1)
        t = jnp.dot(rows, w, preferred_element_type=F32).astype(BF16)
        for i in range(IB):
            for q in range(2):
                e = 2 * b + q
                big[chunk * IB + i, e * S : (e + 1) * S, :] = t[
                    i * S : (i + 1) * S, q * K : (q + 1) * K
                ]

    def right_gradient(chunk, n):
        cot = jnp.concatenate([cot_buf[chunk * IB + i] for i in range(IB)], axis=1)
        back = jnp.concatenate(
            [
                jnp.concatenate(
                    [
                        big[
                            chunk * IB + i, n * 256 + a * 128 : n * 256 + (a + 1) * 128, :
                        ].T
                        for a in range(2)
                    ],
                    axis=1,
                )
                for i in range(IB)
            ],
            axis=0,
        )
        acc_t[:, n * 256 : (n + 1) * 256] += jnp.dot(cot, back, preferred_element_type=F32)

    def both(chunk):
        for n in range(4):
            for b in range(4 * n, 4 * n + 4):
                intermediate(chunk + 1, b)
            right_gradient(chunk, n)

    def two_chunks(g, _):
        both(2 * g)
        both(2 * g + 1)
        return 0

    acc_t[...] = jnp.zeros_like(acc_t)
    for b in range(C // 2):
        intermediate(0, b)
    last = T // IB - 2
    lax.fori_loop(0, last // 2, two_chunks, 0)
    both(last)
    for n in range(4):
        right_gradient(last + 1, n)

    for b in range(8):
        turned[b * 128 : (b + 1) * 128, :] = acc_t[:, b * 128 : (b + 1) * 128].T
    for s in range(S):
        dr_out[s // 2, (s % 2) * C : (s % 2 + 1) * C, :] = turned[
            pl.ds(s, C, stride=S), :
        ].astype(BF16)
    dr_sends = [
        push("wide", me_w, d, dr_out.at[(me_w + d) % N], dr_in, drsend, drrecv)
        for d in NEAR_FIRST
    ]
    for copy in dr_sends:
        copy.start()
    dr_in[me_w] = dr_out[me_w]

    def pairs(t, _):
        rows = jnp.concatenate([rt[b] for b in range(8)], axis=1)
        for p in range(IP // 2):
            i = t * IP + 2 * p
            cols = jnp.concatenate([big[i], big[i + 1]], axis=1)
            out = jnp.dot(rows, cols, preferred_element_type=F32)
            for q in range(2):
                pair_ref[i + q] = (out[:, q * K : (q + 1) * K] + bias_v[...]).astype(BF16)
        return 0

    lax.fori_loop(0, T // IP, pairs, 0)

    for d in range(1, N):
        arrived("narrow", me_n, d, dl_out.at[0], dl_in, dlsend, dlrecv)
    gl_ref[...] = total_of(dl_in)
    for copy in sends + dl_sends:
        copy.wait_send()
    for d in range(1, N):
        arrived("wide", me_w, d, dr_out.at[0], dr_in, drsend, drrecv)
    gr_ref[...] = total_of(dr_in)
    for copy in dr_sends:
        copy.wait_send()


def local(left, right, out_weight, out_bias, cotangent):
    vmem = pl.BlockSpec(memory_space=pltpu.VMEM)
    hbm = pl.BlockSpec(memory_space=pltpu.HBM)
    pin = lambda x: pltpu.with_memory_space_constraint(x, pltpu.HBM)
    pair_update, gl, gr = pl.pallas_call(
        kernel,
        out_shape=(
            jax.ShapeDtypeStruct((T, T, K), BF16),
            jax.ShapeDtypeStruct((64, T), F32),
            jax.ShapeDtypeStruct((64, T), F32),
        ),
        in_specs=[hbm] * 5,
        out_specs=(vmem,) * 3,
        scratch_shapes=[
            pltpu.VMEM((64, T), BF16),
            pltpu.VMEM((64, T), BF16),
            pltpu.VMEM((C * C, K), BF16),
            pltpu.VMEM((1, K), F32),
            pltpu.VMEM((N, 64, T), BF16),
            pltpu.VMEM((N, 64, T), BF16),
            pltpu.VMEM((T, T, K), BF16),
            pltpu.VMEM((C * S, 128), F32),
            pltpu.VMEM((C * S, 128), F32),
            pltpu.VMEM((T * S, 128), F32),
            pltpu.VMEM((T * S, C), BF16),
            pltpu.VMEM((8, T, 128), BF16),
            pltpu.VMEM((C, C, K), BF16),
            pltpu.VMEM((C * C, K), BF16),
            pltpu.VMEM((C * T, S), BF16),
            pltpu.VMEM((T, C * S, 128), BF16),
            pltpu.VMEM((T * C, 128), F32),
            pltpu.VMEM((C * S, 128), F32),
            pltpu.VMEM((T, C * S), F32),
            pltpu.VMEM((N, 64, T), BF16),
            pltpu.VMEM((N, 64, T), BF16),
            pltpu.VMEM((N, 64, T), BF16),
            pltpu.VMEM((N, 64, T), BF16),
            pltpu.SemaphoreType.DMA((4,)),
            pltpu.SemaphoreType.DMA((T // IC,)),
        ]
        + [pltpu.SemaphoreType.DMA((N,))] * 8,
        compiler_params=pltpu.CompilerParams(
            collective_id=0, has_side_effects=True, vmem_limit_bytes=49 << 20
        ),
        name="outer_product_mean",
    )(
        pin(left.reshape(64, T)),
        pin(right.reshape(64, T)),
        pin(out_weight),
        pin(out_bias.reshape(1, K)),
        pin(cotangent),
    )
    return pair_update, gl.reshape(2, C, T), gr.reshape(2, C, T)


def solution(mesh):
    return jax.shard_map(
        local,
        mesh=mesh,
        in_specs=(
            P("narrow", None, "wide"),
            P("wide", None, "narrow"),
            P(),
            P(),
            P("wide", "narrow", None),
        ),
        out_specs=(P("wide", "narrow", None), P("narrow", None, "wide"), P("wide", None, "narrow")),
        check_vma=False,
    )
```

```python
import jax
import jax.numpy as jnp
from jax import lax
from jax.experimental import pallas as pl
from jax.experimental.pallas import tpu as pltpu
from jax.sharding import PartitionSpec as P

F32 = jnp.float32
BF16 = jnp.bfloat16
MESH = pl.DeviceIdType.MESH
NT = (((1,), (1,)), ((), ()))

N = 16
S = 32
C = 32
K = 128
T = 128
IC = 16
IM = 4
GAP = T + 8
IB = 8
IP = 16
AHEAD = 4
LATE = 2
NEAR_FIRST = (1, 15, 8, 2, 14, 9, 7, 3, 13, 10, 6, 4, 12, 11, 5)


def push(axis, me, d, src, dst, send_sem, recv_sem):
    return pltpu.make_async_remote_copy(
        src, dst.at[me], send_sem.at[d], recv_sem.at[me],
        device_id={axis: (me + d) % N}, device_id_type=MESH,
    )


def arrived(axis, me, d, src, dst, send_sem, recv_sem):
    peer = (me + d) % N
    pltpu.make_async_remote_copy(
        src, dst.at[peer], send_sem.at[d], recv_sem.at[peer],
        device_id={axis: peer}, device_id_type=MESH,
    ).wait_recv()


def cot_copy(cot_hbm, cot_buf, sems, t):
    at = pl.multiple_of(t * IC, IC)
    return pltpu.make_async_copy(
        cot_hbm.at[pl.ds(at, IC)], cot_buf.at[pl.ds(at, IC)], sems.at[t]
    )


def total_of(blocks):
    total = blocks[0].astype(F32)
    for n in range(1, N):
        total += blocks[n].astype(F32)
    return total


def kernel(
    left_hbm, right_hbm, w_hbm, bias_hbm, cot_hbm,
    pair_ref, dl_in, dr_in,
    left_v, right_v, w_v, bias_v, l_buf, r_buf, cot_buf, wide_f, left_f, lt_f, lt, rt, w2,
    big, right_l, turned, acc_t, dl_out, dr_out,
    in_sem, cot_sem, lsend, lrecv, rsend, rrecv, dlsend, dlrecv, drsend, drrecv,
):
    me_w = lax.axis_index("wide")
    me_n = lax.axis_index("narrow")
    barrier = pltpu.get_barrier_semaphore()
    for d in range(1, N):
        pl.semaphore_signal(
            barrier, inc=1, device_id={"wide": (me_w + d) % N}, device_id_type=MESH
        )
        pl.semaphore_signal(
            barrier, inc=1, device_id={"narrow": (me_n + d) % N}, device_id_type=MESH
        )
    fetches = [
        pltpu.make_async_copy(src, dst, in_sem.at[n])
        for n, (src, dst) in enumerate(
            ((w_hbm, w_v), (right_hbm, right_v), (left_hbm, left_v), (bias_hbm, bias_v))
        )
    ]
    for copy in fetches:
        copy.start()
    for t in range(T // IC):
        cot_copy(cot_hbm, cot_buf, cot_sem, t).start()

    def turn(t, _):
        cot_copy(cot_hbm, cot_buf, cot_sem, t).wait()
        for i in range(IC):
            lt_f[i * GAP : i * GAP + T, :] = cot_buf[t * IC + i].astype(F32)
        for j in range(T):
            pair_ref[j, pl.ds(pl.multiple_of(t * IC, IC), IC), :] = lt_f[
                pl.ds(j, IC, stride=GAP), :
            ].astype(BF16)
        return 0

    lax.fori_loop(0, T // IC, turn, 0)
    for copy in fetches:
        copy.wait()

    def project(t, _):
        base = t * IC
        for p in range(IC // 2):
            rows = pair_ref[pl.ds(base + 2 * p, 2)].reshape(2 * T, K)
            d = lax.dot_general(w_v[...], rows, NT, preferred_element_type=F32)
            d = d.astype(BF16)
            for q in range(2):
                big[base + 2 * p + q] = d[:, q * T : (q + 1) * T]
        return 0

    lax.fori_loop(0, AHEAD, project, 0)
    pl.semaphore_wait(barrier, 2 * (N - 1))
    sends = [push("wide", me_w, d, right_v, r_buf, rsend, rrecv) for d in NEAR_FIRST]
    sends += [push("narrow", me_n, d, left_v, l_buf, lsend, lrecv) for d in NEAR_FIRST]
    for copy in sends:
        copy.start()
    r_buf[me_w] = right_v[...]
    l_buf[me_n] = left_v[...]
    lax.fori_loop(AHEAD, T // IC, project, 0)

    wide_f[...] = w_v[...].astype(F32)
    for e in range(C):
        w2[e] = wide_f[pl.ds(e, C, stride=C), :].astype(BF16)

    for d in range(1, N):
        arrived("wide", me_w, d, right_v, r_buf, rsend, rrecv)
    for w in range(N):
        wide_f[w * 64 : (w + 1) * 64, :] = r_buf[w].astype(F32)
    for s in range(S):
        lt_f[s * T : (s + 1) * T, 0:C] = wide_f[s * C : (s + 1) * C, :].T
    for s in range(S):
        turned[s * 32 : (s + 1) * 32, :] = jnp.concatenate(
            [lt_f[pl.ds(s * T + m, 32, stride=4), 0:C] for m in range(4)], axis=1
        )
    for b in range(T // 4):
        right_l[b] = turned[pl.ds(b, S, stride=32), :].astype(BF16)

    def left_gradient(t):
        rows = jnp.concatenate([right_l[b] for b in range(T // 4)], axis=1)
        for p in range(IM // 2):
            c = t * IM + 2 * p
            cols = jnp.concatenate(
                [
                    big[:, pl.ds(pl.multiple_of((c + q) * C, C), C), :].reshape(T * C, T)
                    for q in range(2)
                ],
                axis=1,
            )
            out = jnp.dot(rows, cols, preferred_element_type=F32) * (1.0 / S)
            for q in range(2):
                turned[pl.ds(pl.multiple_of((c + q) * S, S), S), :] = out[
                    :, q * T : (q + 1) * T
                ]

    def early(t, _):
        left_gradient(t)
        return 0

    def late(t, _):
        left_gradient(t)
        u = t - (C // IM - LATE)
        for q in range(S // LATE):
            s = u * (S // LATE) + q
            part = left_f[pl.ds(pl.multiple_of(s * C, C), C), :]
            lt_f[pl.ds(s, T, stride=S), 0:C] = part.T
        for q in range(8 // LATE):
            b = u * (8 // LATE) + q
            rows = jnp.concatenate(
                [wide_f[pl.ds(4 * b + m, S, stride=C), :] for m in range(4)], axis=0
            )
            rt[b] = rows.T.astype(BF16)
        return 0

    lax.fori_loop(0, C // IM - LATE, early, 0)
    for d in range(1, N):
        arrived("narrow", me_n, d, left_v, l_buf, lsend, lrecv)
    for n in range(N):
        left_f[n * 64 : (n + 1) * 64, :] = l_buf[n].astype(F32) * (1.0 / S)
    lax.fori_loop(C // IM - LATE, C // IM, late, 0)
    lt[...] = lt_f[:, 0:C].astype(BF16)

    for s in range(S):
        dl_out[s // 2, (s % 2) * C : (s % 2 + 1) * C, :] = turned[
            pl.ds(s, C, stride=S), :
        ].astype(BF16)
    dl_sends = [
        push("narrow", me_n, d, dl_out.at[(me_n + d) % N], dl_in, dlsend, dlrecv)
        for d in NEAR_FIRST
    ]
    for copy in dl_sends:
        copy.start()
    dl_in[me_n] = dl_out[me_n]

    def intermediate(chunk, b):
        rows = lt[pl.ds(pl.multiple_of(chunk * (IB * S), IB * S), IB * S), :]
        w = jnp.concatenate([w2[2 * b], w2[2 * b + 1]], axis=1)
        t = jnp.dot(rows, w, preferred_element_type=F32).astype(BF16)
        for i in range(IB):
            for q in range(2):
                e = 2 * b + q
                big[chunk * IB + i, e * S : (e + 1) * S, :] = t[
                    i * S : (i + 1) * S, q * K : (q + 1) * K
                ]

    def right_gradient(chunk, n):
        cot = jnp.concatenate([cot_buf[chunk * IB + i] for i in range(IB)], axis=1)
        back = jnp.concatenate(
            [
                jnp.concatenate(
                    [
                        big[
                            chunk * IB + i, n * 256 + a * 128 : n * 256 + (a + 1) * 128, :
                        ].T
                        for a in range(2)
                    ],
                    axis=1,
                )
                for i in range(IB)
            ],
            axis=0,
        )
        acc_t[:, n * 256 : (n + 1) * 256] += jnp.dot(cot, back, preferred_element_type=F32)

    def both(chunk):
        for n in range(4):
            for b in range(4 * n, 4 * n + 4):
                intermediate(chunk + 1, b)
            right_gradient(chunk, n)

    def two_chunks(g, _):
        both(2 * g)
        both(2 * g + 1)
        return 0

    acc_t[...] = jnp.zeros_like(acc_t)
    for b in range(C // 2):
        intermediate(0, b)
    last = T // IB - 2
    lax.fori_loop(0, last // 2, two_chunks, 0)
    both(last)
    for n in range(4):
        right_gradient(last + 1, n)

    for b in range(8):
        turned[b * 128 : (b + 1) * 128, :] = acc_t[:, b * 128 : (b + 1) * 128].T
    for s in range(S):
        dr_out[s // 2, (s % 2) * C : (s % 2 + 1) * C, :] = turned[
            pl.ds(s, C, stride=S), :
        ].astype(BF16)
    dr_sends = [
        push("wide", me_w, d, dr_out.at[(me_w + d) % N], dr_in, drsend, drrecv)
        for d in NEAR_FIRST
    ]
    for copy in dr_sends:
        copy.start()
    dr_in[me_w] = dr_out[me_w]

    def pairs(t, _):
        rows = jnp.concatenate([rt[b] for b in range(8)], axis=1)
        for p in range(IP // 2):
            i = t * IP + 2 * p
            cols = jnp.concatenate([big[i], big[i + 1]], axis=1)
            out = jnp.dot(rows, cols, preferred_element_type=F32)
            for q in range(2):
                pair_ref[i + q] = (out[:, q * K : (q + 1) * K] + bias_v[...]).astype(BF16)
        return 0

    lax.fori_loop(0, T // IP, pairs, 0)

    for d in range(1, N):
        arrived("narrow", me_n, d, dl_out.at[0], dl_in, dlsend, dlrecv)
    for copy in sends + dl_sends:
        copy.wait_send()
    for d in range(1, N):
        arrived("wide", me_w, d, dr_out.at[0], dr_in, drsend, drrecv)
    for copy in dr_sends:
        copy.wait_send()


def finish_kernel(
    pair_v, dl_in, dr_in, pair_hbm, gl_hbm, gr_hbm, gl_v, gr_v, sems
):
    part = T // 4
    copies = [
        pltpu.make_async_copy(
            pair_v.at[pl.ds(n * part, part)], pair_hbm.at[pl.ds(n * part, part)], sems.at[n]
        )
        for n in range(4)
    ]
    for copy in copies:
        copy.start()
    for blocks, total, out, n in ((dl_in, gl_v, gl_hbm, 4), (dr_in, gr_v, gr_hbm, 5)):
        total[...] = total_of(blocks).reshape(2, C, T)
        copies.append(pltpu.make_async_copy(total, out, sems.at[n]))
        copies[-1].start()
    for copy in copies:
        copy.wait()


def local(left, right, out_weight, out_bias, cotangent):
    vmem = pl.BlockSpec(memory_space=pltpu.VMEM)
    hbm = pl.BlockSpec(memory_space=pltpu.HBM)
    pin = lambda x: pltpu.with_memory_space_constraint(x, pltpu.HBM)
    pair_v, dl, dr = pl.pallas_call(
        kernel,
        out_shape=(
            jax.ShapeDtypeStruct((T, T, K), BF16),
            jax.ShapeDtypeStruct((N, 64, T), BF16),
            jax.ShapeDtypeStruct((N, 64, T), BF16),
        ),
        in_specs=[hbm] * 5,
        out_specs=(vmem,) * 3,
        scratch_shapes=[
            pltpu.VMEM((64, T), BF16),
            pltpu.VMEM((64, T), BF16),
            pltpu.VMEM((C * C, K), BF16),
            pltpu.VMEM((1, K), F32),
            pltpu.VMEM((N, 64, T), BF16),
            pltpu.VMEM((N, 64, T), BF16),
            pltpu.VMEM((T, T, K), BF16),
            pltpu.VMEM((C * S, 128), F32),
            pltpu.VMEM((C * S, 128), F32),
            pltpu.VMEM((T * S, 128), F32),
            pltpu.VMEM((T * S, C), BF16),
            pltpu.VMEM((8, T, 128), BF16),
            pltpu.VMEM((C, C, K), BF16),
            pltpu.VMEM((T, C * S, 128), BF16),
            pltpu.VMEM((T // 4, S, 128), BF16),
            pltpu.VMEM((C * S, 128), F32),
            pltpu.VMEM((T, C * S), F32),
            pltpu.VMEM((N, 64, T), BF16),
            pltpu.VMEM((N, 64, T), BF16),
            pltpu.SemaphoreType.DMA((4,)),
            pltpu.SemaphoreType.DMA((T // IC,)),
        ]
        + [pltpu.SemaphoreType.DMA((N,))] * 8,
        compiler_params=pltpu.CompilerParams(
            collective_id=0, has_side_effects=True, vmem_limit_bytes=49 << 20
        ),
        name="outer_product_mean",
    )(
        pin(left.reshape(64, T)),
        pin(right.reshape(64, T)),
        pin(out_weight),
        pin(out_bias.reshape(1, K)),
        pin(cotangent),
    )
    return pl.pallas_call(
        finish_kernel,
        out_shape=(
            jax.ShapeDtypeStruct((T, T, K), BF16),
            jax.ShapeDtypeStruct((2, C, T), F32),
            jax.ShapeDtypeStruct((2, C, T), F32),
        ),
        in_specs=[vmem] * 3,
        out_specs=(hbm,) * 3,
        scratch_shapes=[
            pltpu.VMEM((2, C, T), F32),
            pltpu.VMEM((2, C, T), F32),
            pltpu.SemaphoreType.DMA((6,)),
        ],
        compiler_params=pltpu.CompilerParams(vmem_limit_bytes=4 << 20),
        name="finish",
    )(pair_v, dl, dr)


def solution(mesh):
    return jax.shard_map(
        local,
        mesh=mesh,
        in_specs=(
            P("narrow", None, "wide"),
            P("wide", None, "narrow"),
            P(),
            P(),
            P("wide", "narrow", None),
        ),
        out_specs=(P("wide", "narrow", None), P("narrow", None, "wide"), P("wide", None, "narrow")),
        check_vma=False,
    )
```

```python
import jax
import jax.numpy as jnp
from jax import lax
from jax.experimental import pallas as pl
from jax.experimental.pallas import tpu as pltpu
from jax.sharding import PartitionSpec as P

F32 = jnp.float32
BF16 = jnp.bfloat16
MESH = pl.DeviceIdType.MESH
NT = (((1,), (1,)), ((), ()))

N = 16
S = 32
C = 32
K = 128
T = 128
IC = 16
IM = 4
GAP = T + 8
IB = 8
IP = 16
AHEAD = 2
LATE = 2
NEAR_FIRST = (1, 15, 8, 2, 14, 9, 7, 3, 13, 10, 6, 4, 12, 11, 5)


def push(axis, me, d, src, dst, send_sem, recv_sem):
    return pltpu.make_async_remote_copy(
        src, dst.at[me], send_sem.at[d], recv_sem.at[me],
        device_id={axis: (me + d) % N}, device_id_type=MESH,
    )


def arrived(axis, me, d, src, dst, send_sem, recv_sem):
    peer = (me + d) % N
    pltpu.make_async_remote_copy(
        src, dst.at[peer], send_sem.at[d], recv_sem.at[peer],
        device_id={axis: peer}, device_id_type=MESH,
    ).wait_recv()


def cot_copy(cot_hbm, cot_buf, sems, t):
    at = pl.multiple_of(t * IC, IC)
    return pltpu.make_async_copy(
        cot_hbm.at[pl.ds(at, IC)], cot_buf.at[pl.ds(at, IC)], sems.at[t]
    )


def total_of(blocks):
    total = blocks[0].astype(F32)
    for n in range(1, N):
        total += blocks[n].astype(F32)
    return total


def kernel(
    left_hbm, right_hbm, w_hbm, bias_hbm, cot_hbm,
    pair_ref, dl_in, dr_in,
    left_v, right_v, w_v, bias_v, l_buf, r_buf, cot_buf, wide_f, left_f, lt_f, lt, rt, w2,
    big, right_l, turned, acc_t, dl_out, dr_out,
    in_sem, cot_sem, lsend, lrecv, rsend, rrecv, dlsend, dlrecv, drsend, drrecv,
):
    me_w = lax.axis_index("wide")
    me_n = lax.axis_index("narrow")
    barrier = pltpu.get_barrier_semaphore()
    for d in range(1, N):
        pl.semaphore_signal(
            barrier, inc=1, device_id={"wide": (me_w + d) % N}, device_id_type=MESH
        )
        pl.semaphore_signal(
            barrier, inc=1, device_id={"narrow": (me_n + d) % N}, device_id_type=MESH
        )
    fetches = [
        pltpu.make_async_copy(src, dst, in_sem.at[n])
        for n, (src, dst) in enumerate(
            ((w_hbm, w_v), (right_hbm, right_v), (left_hbm, left_v), (bias_hbm, bias_v))
        )
    ]
    for copy in fetches:
        copy.start()
    for t in range(T // IC):
        cot_copy(cot_hbm, cot_buf, cot_sem, t).start()

    def turn(t, _):
        cot_copy(cot_hbm, cot_buf, cot_sem, t).wait()
        for i in range(IC):
            lt_f[i * GAP : i * GAP + T, :] = cot_buf[t * IC + i].astype(F32)
        for j in range(T):
            pair_ref[j, pl.ds(pl.multiple_of(t * IC, IC), IC), :] = lt_f[
                pl.ds(j, IC, stride=GAP), :
            ].astype(BF16)
        return 0

    lax.fori_loop(0, T // IC, turn, 0)
    for copy in fetches:
        copy.wait()

    def project(t, _):
        base = t * IC
        for p in range(IC // 2):
            rows = pair_ref[pl.ds(base + 2 * p, 2)].reshape(2 * T, K)
            d = lax.dot_general(w_v[...], rows, NT, preferred_element_type=F32)
            d = d.astype(BF16)
            for q in range(2):
                big[base + 2 * p + q] = d[:, q * T : (q + 1) * T]
        return 0

    lax.fori_loop(0, AHEAD, project, 0)
    pl.semaphore_wait(barrier, 2 * (N - 1))
    sends = [push("wide", me_w, d, right_v, r_buf, rsend, rrecv) for d in NEAR_FIRST]
    sends += [push("narrow", me_n, d, left_v, l_buf, lsend, lrecv) for d in NEAR_FIRST]
    for copy in sends:
        copy.start()
    r_buf[me_w] = right_v[...]
    l_buf[me_n] = left_v[...]
    lax.fori_loop(AHEAD, T // IC, project, 0)

    wide_f[...] = w_v[...].astype(F32)
    for e in range(C):
        w2[e] = wide_f[pl.ds(e, C, stride=C), :].astype(BF16)

    for d in range(1, N):
        arrived("wide", me_w, d, right_v, r_buf, rsend, rrecv)
    for w in range(N):
        wide_f[w * 64 : (w + 1) * 64, :] = r_buf[w].astype(F32)
    for s in range(S):
        lt_f[s * T : (s + 1) * T, 0:C] = wide_f[s * C : (s + 1) * C, :].T
    for s in range(S):
        turned[s * 32 : (s + 1) * 32, :] = jnp.concatenate(
            [lt_f[pl.ds(s * T + m, 32, stride=4), 0:C] for m in range(4)], axis=1
        )
    for b in range(T // 4):
        right_l[b] = turned[pl.ds(b, S, stride=32), :].astype(BF16)

    def left_gradient(t):
        rows = jnp.concatenate([right_l[b] for b in range(T // 4)], axis=1)
        for p in range(IM // 2):
            c = t * IM + 2 * p
            cols = jnp.concatenate(
                [
                    big[:, pl.ds(pl.multiple_of((c + q) * C, C), C), :].reshape(T * C, T)
                    for q in range(2)
                ],
                axis=1,
            )
            out = jnp.dot(rows, cols, preferred_element_type=F32) * (1.0 / S)
            for q in range(2):
                turned[pl.ds(pl.multiple_of((c + q) * S, S), S), :] = out[
                    :, q * T : (q + 1) * T
                ]

    def early(t, _):
        left_gradient(t)
        return 0

    def late(t, _):
        left_gradient(t)
        u = t - (C // IM - LATE)
        for q in range(S // LATE):
            s = u * (S // LATE) + q
            part = left_f[pl.ds(pl.multiple_of(s * C, C), C), :]
            lt_f[pl.ds(s, T, stride=S), 0:C] = part.T
        for q in range(8 // LATE):
            b = u * (8 // LATE) + q
            rows = jnp.concatenate(
                [wide_f[pl.ds(4 * b + m, S, stride=C), :] for m in range(4)], axis=0
            )
            rt[b] = rows.T.astype(BF16)
        return 0

    lax.fori_loop(0, C // IM - LATE, early, 0)
    for d in range(1, N):
        arrived("narrow", me_n, d, left_v, l_buf, lsend, lrecv)
    for n in range(N):
        left_f[n * 64 : (n + 1) * 64, :] = l_buf[n].astype(F32) * (1.0 / S)
    lax.fori_loop(C // IM - LATE, C // IM, late, 0)
    lt[...] = lt_f[:, 0:C].astype(BF16)

    for s in range(S):
        dl_out[s // 2, (s % 2) * C : (s % 2 + 1) * C, :] = turned[
            pl.ds(s, C, stride=S), :
        ].astype(BF16)
    dl_sends = [
        push("narrow", me_n, d, dl_out.at[(me_n + d) % N], dl_in, dlsend, dlrecv)
        for d in NEAR_FIRST
    ]
    for copy in dl_sends:
        copy.start()
    dl_in[me_n] = dl_out[me_n]

    def intermediate(chunk, b):
        rows = lt[pl.ds(pl.multiple_of(chunk * (IB * S), IB * S), IB * S), :]
        w = jnp.concatenate([w2[2 * b], w2[2 * b + 1]], axis=1)
        t = jnp.dot(rows, w, preferred_element_type=F32).astype(BF16)
        for i in range(IB):
            for q in range(2):
                e = 2 * b + q
                big[chunk * IB + i, e * S : (e + 1) * S, :] = t[
                    i * S : (i + 1) * S, q * K : (q + 1) * K
                ]

    def right_gradient(chunk, n):
        cot = jnp.concatenate([cot_buf[chunk * IB + i] for i in range(IB)], axis=1)
        back = jnp.concatenate(
            [
                jnp.concatenate(
                    [
                        big[
                            chunk * IB + i, n * 256 + a * 128 : n * 256 + (a + 1) * 128, :
                        ].T
                        for a in range(2)
                    ],
                    axis=1,
                )
                for i in range(IB)
            ],
            axis=0,
        )
        acc_t[:, n * 256 : (n + 1) * 256] += jnp.dot(cot, back, preferred_element_type=F32)

    def both(chunk):
        for n in range(4):
            for b in range(4 * n, 4 * n + 4):
                intermediate(chunk + 1, b)
            right_gradient(chunk, n)

    def two_chunks(g, _):
        both(2 * g)
        both(2 * g + 1)
        return 0

    acc_t[...] = jnp.zeros_like(acc_t)
    for b in range(C // 2):
        intermediate(0, b)
    last = T // IB - 2
    lax.fori_loop(0, last // 2, two_chunks, 0)
    both(last)
    for n in range(4):
        right_gradient(last + 1, n)

    for b in range(8):
        turned[b * 128 : (b + 1) * 128, :] = acc_t[:, b * 128 : (b + 1) * 128].T
    for s in range(S):
        dr_out[s // 2, (s % 2) * C : (s % 2 + 1) * C, :] = turned[
            pl.ds(s, C, stride=S), :
        ].astype(BF16)
    dr_sends = [
        push("wide", me_w, d, dr_out.at[(me_w + d) % N], dr_in, drsend, drrecv)
        for d in NEAR_FIRST
    ]
    for copy in dr_sends:
        copy.start()
    dr_in[me_w] = dr_out[me_w]

    def pairs(t, _):
        rows = jnp.concatenate([rt[b] for b in range(8)], axis=1)
        for p in range(IP // 2):
            i = t * IP + 2 * p
            cols = jnp.concatenate([big[i], big[i + 1]], axis=1)
            out = jnp.dot(rows, cols, preferred_element_type=F32)
            for q in range(2):
                pair_ref[i + q] = (out[:, q * K : (q + 1) * K] + bias_v[...]).astype(BF16)
        return 0

    lax.fori_loop(0, T // IP, pairs, 0)

    for d in range(1, N):
        arrived("narrow", me_n, d, dl_out.at[0], dl_in, dlsend, dlrecv)
    for copy in sends + dl_sends:
        copy.wait_send()
    for d in range(1, N):
        arrived("wide", me_w, d, dr_out.at[0], dr_in, drsend, drrecv)
    for copy in dr_sends:
        copy.wait_send()


def finish_kernel(
    pair_v, dl_in, dr_in, pair_hbm, gl_hbm, gr_hbm, gl_v, gr_v, sems
):
    part = T // 4
    copies = [
        pltpu.make_async_copy(
            pair_v.at[pl.ds(n * part, part)], pair_hbm.at[pl.ds(n * part, part)], sems.at[n]
        )
        for n in range(4)
    ]
    for copy in copies:
        copy.start()
    for blocks, total, out, n in ((dl_in, gl_v, gl_hbm, 4), (dr_in, gr_v, gr_hbm, 5)):
        total[...] = total_of(blocks).reshape(2, C, T)
        copies.append(pltpu.make_async_copy(total, out, sems.at[n]))
        copies[-1].start()
    for copy in copies:
        copy.wait()


def local(left, right, out_weight, out_bias, cotangent):
    vmem = pl.BlockSpec(memory_space=pltpu.VMEM)
    hbm = pl.BlockSpec(memory_space=pltpu.HBM)
    pin = lambda x: pltpu.with_memory_space_constraint(x, pltpu.HBM)
    pair_v, dl, dr = pl.pallas_call(
        kernel,
        out_shape=(
            jax.ShapeDtypeStruct((T, T, K), BF16),
            jax.ShapeDtypeStruct((N, 64, T), BF16),
            jax.ShapeDtypeStruct((N, 64, T), BF16),
        ),
        in_specs=[hbm] * 5,
        out_specs=(vmem,) * 3,
        scratch_shapes=[
            pltpu.VMEM((64, T), BF16),
            pltpu.VMEM((64, T), BF16),
            pltpu.VMEM((C * C, K), BF16),
            pltpu.VMEM((1, K), F32),
            pltpu.VMEM((N, 64, T), BF16),
            pltpu.VMEM((N, 64, T), BF16),
            pltpu.VMEM((T, T, K), BF16),
            pltpu.VMEM((C * S, 128), F32),
            pltpu.VMEM((C * S, 128), F32),
            pltpu.VMEM((T * S, 128), F32),
            pltpu.VMEM((T * S, C), BF16),
            pltpu.VMEM((8, T, 128), BF16),
            pltpu.VMEM((C, C, K), BF16),
            pltpu.VMEM((T, C * S, 128), BF16),
            pltpu.VMEM((T // 4, S, 128), BF16),
            pltpu.VMEM((C * S, 128), F32),
            pltpu.VMEM((T, C * S), F32),
            pltpu.VMEM((N, 64, T), BF16),
            pltpu.VMEM((N, 64, T), BF16),
            pltpu.SemaphoreType.DMA((4,)),
            pltpu.SemaphoreType.DMA((T // IC,)),
        ]
        + [pltpu.SemaphoreType.DMA((N,))] * 8,
        compiler_params=pltpu.CompilerParams(
            collective_id=0, has_side_effects=True, vmem_limit_bytes=49 << 20
        ),
        name="outer_product_mean",
    )(
        pin(left.reshape(64, T)),
        pin(right.reshape(64, T)),
        pin(out_weight),
        pin(out_bias.reshape(1, K)),
        pin(cotangent),
    )
    return pl.pallas_call(
        finish_kernel,
        out_shape=(
            jax.ShapeDtypeStruct((T, T, K), BF16),
            jax.ShapeDtypeStruct((2, C, T), F32),
            jax.ShapeDtypeStruct((2, C, T), F32),
        ),
        in_specs=[vmem] * 3,
        out_specs=(hbm,) * 3,
        scratch_shapes=[
            pltpu.VMEM((2, C, T), F32),
            pltpu.VMEM((2, C, T), F32),
            pltpu.SemaphoreType.DMA((6,)),
        ],
        compiler_params=pltpu.CompilerParams(vmem_limit_bytes=4 << 20),
        name="finish",
    )(pair_v, dl, dr)


def solution(mesh):
    return jax.shard_map(
        local,
        mesh=mesh,
        in_specs=(
            P("narrow", None, "wide"),
            P("wide", None, "narrow"),
            P(),
            P(),
            P("wide", "narrow", None),
        ),
        out_specs=(P("wide", "narrow", None), P("narrow", None, "wide"), P("wide", None, "narrow")),
        check_vma=False,
    )
```
